512 devices in a mesh: groups: 2 (over y), batch: 128 (over z, x), mp: 2 (over core).
Axes of the slice: x: 4, y: 2, z: 32, core: 2. Of those that a mesh axis runs over, the one named last changes fastest.
The devices are a block of a 4x8x32 slice.
Arguments:
- hidden: bfloat16 [512, 1280], P(('groups', 'batch')), parts along dimension 0, may hold values from -6 to 6
- token_qkv: bfloat16 [3, 512, 1280], P(None, ('groups', 'batch'), 'mp'), parts along dimension 1, may hold values from -6 to 6
- self_cache: bfloat16 [2, 512, 128, 1280], P(None, ('groups', 'batch'), None, 'mp'), parts along dimension 1, may hold values from -6 to 6
- cross_kv: bfloat16 [2, 512, 64, 1280], P(None, ('groups', 'batch'), None, 'mp'), parts along dimension 1, may hold values from -6 to 6
- cache_len: int32 [512], P(('groups', 'batch')), parts along dimension 0, may hold values from 1 to 127
- finished: int32 [512], P(('groups', 'batch')), parts along dimension 0, may hold values 0 or 1
- new_slot: int32 [512], P(('groups', 'batch')), parts along dimension 0, may hold values from 0 to 255, as said below
- out_proj: bfloat16 [1280, 1280], P('mp'), may hold values from -0.15625 to 0.15625
- ln_gain: float32 [1280], replicated, may hold values from 0.5 to 1.5
- ln_bias: float32 [1280], replicated, may hold values from -3 to 3
- query_proj: bfloat16 [1280, 1280], P(None, 'mp'), may hold values from -3 to 3
Outputs:
- moved_cache: bfloat16 [2, 512, 128, 1280], P(None, ('groups', 'batch'), None, 'mp'), parts along dimension 1
- moved_out: bfloat16 [512, 1280], P(('groups', 'batch'), 'mp'), parts along dimension 0
The draws below stay inside these ranges and needn't reach their ends.
There are 2 independent parts, one for each index of `groups`. The reference program is written for one: setup_inputs(seed, part) draws one part's arguments, and reference() takes and returns one part's arrays. A program takes and returns all parts, laid end to end along the dimension named above; an argument that names none is the same for every part. Nothing has to cross between parts.
Inputs may be any that keep to these rules, and one draw needn't show every extreme that they name: A permutation of the spans' slots. Span c's new owner new_slot[c] // 2 lies within 3 devices of its present one c // 2, counting the device order as a loop; of one device's spans at most one moves by any given signed distance.
All inputs are finite; a program needn't handle non-finite values. No bound on the sum of `finished` on one device may be relied on, other than what follows from the above.
Results may differ from the reference program's by a relative error of at most 0.015.
Values may be sent and summed in bfloat16 or wider, within the bound.
No kernel may reach another device: no remote copies, remote signals or barrier semaphores. Data moves between devices by JAX's collectives and lax.ppermute only.
A program may use at most 64 MiB of HBM per device.

```python
import jax
import jax.numpy as jnp
from jax import lax

D = 1280
HEADS = 20
HEAD_DIM = 64
CH_DEV = 2
ENC = 64
SLOTS = 128
SPANS = 256


def swap_round(key, table, stride, period):
    devices, width = table.shape
    keys = jax.random.split(key, 4)
    phase = jax.random.randint(keys[0], (), 0, period)
    left_slot = jax.random.randint(keys[1], (devices,), 0, width)
    right_slot = jax.random.randint(keys[2], (devices,), 0, width)
    coin = jax.random.randint(keys[3], (devices,), 0, 2)
    index = jnp.arange(devices, dtype=jnp.int32)
    is_left = (index - phase) % period < stride
    partner = jnp.where(is_left, (index + stride) % devices, (index - stride) % devices)
    leader = jnp.where(is_left, index, partner)
    mine = jnp.where(is_left, left_slot[leader], right_slot[leader])
    theirs = jnp.where(is_left, right_slot[leader], left_slot[leader])
    swapping = coin[leader] == 1
    incoming = table[partner, theirs]
    column = jnp.arange(width, dtype=jnp.int32)[None, :] == mine[:, None]
    return jnp.where(column & swapping[:, None], incoming[:, None], table)


def draw_new_slot(key, part):
    devices = SPANS // CH_DEV
    table = jnp.arange(SPANS, dtype=jnp.int32).reshape(devices, CH_DEV)
    table = swap_round(jax.random.fold_in(key, 11), table, 1, 2)
    table = swap_round(jax.random.fold_in(key, 12), table, 2, 4)
    return jnp.zeros((SPANS,), jnp.int32).at[table.reshape(-1)].set(jnp.arange(SPANS, dtype=jnp.int32))


def rough_noise(key, shape):
    return jax.random.truncated_normal(key, -6.0, 6.0, shape, jnp.float32)


def fixed_pattern():
    dims = jnp.arange(HEAD_DIM, dtype=jnp.int32)
    return jnp.where((dims * 37 + 11) % 8 < 4, 1.0, -1.0).astype(jnp.float32)


def self_plan(key):
    keys = jax.random.split(jax.random.fold_in(key, 71), 7)
    span_index = jnp.arange(SPANS, dtype=jnp.int32)[:, None]
    head_index = jnp.arange(HEADS, dtype=jnp.int32)[None, :]
    first_span = jax.random.randint(keys[0], (), 0, SPANS)
    first_head = jax.random.randint(keys[1], (), 0, HEADS)
    forced = (span_index == first_span) & (head_index == first_head)
    planted = (jax.random.randint(keys[2], (SPANS, HEADS), 0, 16) == 0) | forced
    signs = (2 * jax.random.randint(keys[3], (SPANS, HEADS, HEAD_DIM), 0, 2) - 1).astype(jnp.float32)
    query_steps = jnp.where(forced, 185, jax.random.randint(keys[4], (SPANS, HEADS), 112, 186))
    key_steps = jnp.where(forced, 185, jax.random.randint(keys[5], (SPANS, HEADS), 144, 186))
    own_first = jax.random.randint(keys[6], (SPANS, HEADS), 0, 2) == 1
    higher = key_steps.astype(jnp.float32) / 32.0
    lower = (key_steps - 2).astype(jnp.float32) / 32.0
    query_scale = query_steps.astype(jnp.float32) / 32.0
    own_scale = jnp.where(own_first, higher, lower)
    cached_scale = jnp.where(own_first, lower, higher)
    return (planted, signs, query_scale, own_scale, cached_scale)


def draw_token_qkv(key, part):
    base = rough_noise(jax.random.fold_in(key, 1), (3, SPANS, HEADS, HEAD_DIM))
    planted, signs, query_scale, own_scale, cached_scale = self_plan(key)
    mask = planted[:, :, None]
    query_part = jnp.where(mask, query_scale[:, :, None] * signs, base[0])
    key_part = jnp.where(mask, own_scale[:, :, None] * signs, base[1])
    stacked = jnp.stack([query_part, key_part, base[2]])
    return stacked.reshape(3, SPANS, D).astype(jnp.bfloat16)


def draw_self_cache(key, part):
    base = rough_noise(jax.random.fold_in(key, 2), (2, SPANS, SLOTS, HEADS, HEAD_DIM))
    planted, signs, query_scale, own_scale, cached_scale = self_plan(key)
    first_keys = jnp.where(planted[:, :, None], cached_scale[:, :, None] * signs, base[0, :, 0])
    base = base.at[0, :, 0].set(first_keys)
    return base.reshape(2, SPANS, SLOTS, D).astype(jnp.bfloat16)


def draw_cross_kv(key, part):
    base = rough_noise(jax.random.fold_in(key, 3), (2, SPANS, ENC, HEADS, HEAD_DIM))
    keys = jax.random.split(jax.random.fold_in(key, 73), 5)
    span_index = jnp.arange(SPANS, dtype=jnp.int32)
    forced_span = jax.random.randint(keys[0], (), 0, SPANS)
    planted = (jax.random.randint(keys[1], (SPANS,), 0, 8) == 0) | (span_index == forced_span)
    first_frame = jax.random.randint(keys[2], (SPANS,), 0, ENC)
    second_frame = (first_frame + 1 + jax.random.randint(keys[3], (SPANS,), 0, ENC - 1)) % ENC
    key_steps = jnp.where(span_index == forced_span, 184, jax.random.randint(keys[4], (SPANS,), 96, 186))
    higher = key_steps.astype(jnp.float32) / 32.0
    lower = (key_steps - 2).astype(jnp.float32) / 32.0
    frame = jnp.arange(ENC, dtype=jnp.int32)[None, :]
    at_first = frame == first_frame[:, None]
    at_second = frame == second_frame[:, None]
    scale = jnp.where(at_first, higher[:, None], jnp.where(at_second, lower[:, None], 0.0))
    use = planted[:, None] & (at_first | at_second)
    pattern = fixed_pattern()
    key_part = jnp.where(use[:, :, None, None], scale[:, :, None, None] * pattern[None, None, None, :], base[0])
    stacked = jnp.stack([key_part, base[1]])
    return stacked.reshape(2, SPANS, ENC, D).astype(jnp.bfloat16)


def bias_plan(key):
    keys = jax.random.split(jax.random.fold_in(key, 91), 3)
    bias = 0.5 * jax.random.truncated_normal(keys[0], -6.0, 6.0, (D,), jnp.float32)
    head_index = jnp.arange(HEADS, dtype=jnp.int32)
    chosen_head = jax.random.randint(keys[1], (), 0, HEADS)
    heads_on = (jax.random.randint(keys[2], (HEADS,), 0, 4) == 0) | (head_index == chosen_head)
    return (bias, heads_on)


def draw_ln_bias(key, part):
    bias, heads_on = bias_plan(key)
    return bias


def draw_query_proj(key, part):
    bias, heads_on = bias_plan(key)
    weight_key = jax.random.fold_in(key, 92)
    weight = jax.random.truncated_normal(weight_key, -6.0, 6.0, (D, D), jnp.float32) * D ** (-0.5)
    direction = 5.0 * jnp.where(heads_on[:, None], fixed_pattern()[None, :], 0.0).reshape(D)
    norm_sq = jnp.maximum(jnp.sum(bias * bias), D / 8.0)
    weight = weight + (bias / norm_sq)[:, None] * direction[None, :]
    return weight.astype(jnp.bfloat16)


def set_ends(drawn, own_key, low, high):
    extent = drawn.shape
    place = [jax.random.randint(jax.random.fold_in(own_key, axis), (), 0, extent[axis]) for axis in range(len(extent))]
    drawn = drawn.at[tuple(place)].set(low)
    longest = extent.index(max(extent))
    place[longest] = (place[longest] + 1) % extent[longest]
    return drawn.at[tuple(place)].set(high)


def shard_levels(key, shape, shards, low, top_value):
    factor_of, own = 1.0, jax.random.fold_in(key, 6)
    for dim, shards_of in shards:
        heights = jnp.exp(jax.random.uniform(jax.random.fold_in(own, dim), (shards_of,), jnp.float32, low / len(shards), top_value / len(shards)))
        factor_of = factor_of * jnp.repeat(heights, shape[dim] // shards_of).reshape([-1 if axis == dim else 1 for axis in range(len(shape))])
    return factor_of


def noise(key, extent, deviation, reach, shards=(), kind=jnp.bfloat16):
    values = deviation * jax.random.normal(key, extent, jnp.float32)
    if shards:
        values = values * shard_levels(key, extent, shards, -0.22, 0.18)
    return jnp.clip(values, -reach, reach).astype(kind)


def setup_inputs(seed: int = 0, part: int = 0) -> dict:
    seeds = jax.random.split(jax.random.key(seed), 12)
    part_splits = jax.random.split(jax.random.fold_in(seeds[11], part), 12)
    return {
        "hidden": noise(part_splits[0], (SPANS, D), 1.0, 6.0, ((0, 128),)),
        "token_qkv": draw_token_qkv(jax.random.fold_in(jax.random.fold_in(seeds[11], part), 71), part),
        "self_cache": draw_self_cache(jax.random.fold_in(jax.random.fold_in(seeds[11], part), 71), part),
        "cross_kv": draw_cross_kv(jax.random.fold_in(jax.random.fold_in(seeds[11], part), 71), part),
        "cache_len": set_ends(jax.random.randint(part_splits[4], (SPANS,), 1, SLOTS), jax.random.fold_in(part_splits[4], 1), 1, SLOTS - 1).astype(jnp.int32),
        "finished": set_ends((jax.random.randint(part_splits[5], (SPANS,), 0, 4) < 1).astype(jnp.int32), jax.random.fold_in(part_splits[5], 1), 0, 1),
        "new_slot": draw_new_slot(jax.random.fold_in(jax.random.fold_in(seeds[11], part), 71), part),
        "out_proj": noise(seeds[7], (D, D), D ** -0.5, 0.15625, ((0, 2),)),
        "ln_gain": jnp.clip(1.0 + 0.1 * jax.random.normal(seeds[8], (D,), jnp.float32), 0.5, 1.5),
        "ln_bias": draw_ln_bias(jax.random.fold_in(seeds[11], 71), part),
        "query_proj": draw_query_proj(jax.random.fold_in(seeds[11], 71), part),
    }


def reference(hidden, token_qkv, self_cache, cross_kv, cache_len, finished, new_slot, out_proj, ln_gain, ln_bias, query_proj):
    head_count = D // HEAD_DIM
    factor = HEAD_DIM ** (-0.5)
    new_query = token_qkv[0].astype(jnp.float32).reshape(SPANS, head_count, HEAD_DIM)
    new_key = token_qkv[1].astype(jnp.float32).reshape(SPANS, head_count, HEAD_DIM)
    new_value = token_qkv[2].astype(jnp.float32).reshape(SPANS, head_count, HEAD_DIM)
    cache_keys = self_cache[0].astype(jnp.float32).reshape(SPANS, SLOTS, head_count, HEAD_DIM)
    cache_values = self_cache[1].astype(jnp.float32).reshape(SPANS, SLOTS, head_count, HEAD_DIM)
    scores = jnp.einsum('chd,cthd->cht', new_query, cache_keys) * factor
    position = jnp.arange(SLOTS, dtype=jnp.int32)
    usable = position[None, None, :] < cache_len[:, None, None]
    scores = jnp.where(usable, scores, -1e+30)
    own_score = lax.optimization_barrier(jnp.sum(new_query * new_key, axis=-1)) * factor
    highest = jnp.maximum(lax.optimization_barrier(jnp.max(scores, axis=-1)), own_score)
    cache_weight = jnp.where(usable, jnp.exp(scores - highest[..., None]), 0.0)
    own_weight = jnp.exp(own_score - highest)
    total = lax.optimization_barrier(jnp.sum(cache_weight, axis=-1)) + own_weight
    cache_weight = (cache_weight / total[..., None]).astype(jnp.bfloat16)
    own_weight = (own_weight / total).astype(jnp.bfloat16)
    context = jnp.einsum('cht,cthd->chd', cache_weight.astype(jnp.float32), cache_values)
    context = context + own_weight.astype(jnp.float32)[..., None] * new_value
    context = context.astype(jnp.bfloat16).reshape(SPANS, D)
    resid = hidden.astype(jnp.float32) + jnp.dot(context, out_proj, preferred_element_type=jnp.float32)
    centre = lax.optimization_barrier(jnp.mean(resid, axis=-1, keepdims=True))
    spread = lax.optimization_barrier(jnp.mean((resid - centre) ** 2, axis=-1, keepdims=True))
    normed = ((resid - centre) * lax.rsqrt(spread + 1e-05) * ln_gain + ln_bias).astype(jnp.bfloat16)
    cross_query = jnp.dot(normed, query_proj, preferred_element_type=jnp.float32).astype(jnp.bfloat16)
    cross_query = cross_query.astype(jnp.float32).reshape(SPANS, head_count, HEAD_DIM)
    cross_keys = cross_kv[0].astype(jnp.float32).reshape(SPANS, ENC, head_count, HEAD_DIM)
    cross_values = cross_kv[1].astype(jnp.float32).reshape(SPANS, ENC, head_count, HEAD_DIM)
    cross_scores = jnp.einsum('chd,cthd->cht', cross_query, cross_keys) * factor
    cross_high = lax.optimization_barrier(jnp.max(cross_scores, axis=-1, keepdims=True))
    cross_exp = jnp.exp(cross_scores - cross_high)
    cross_weight = (cross_exp / lax.optimization_barrier(jnp.sum(cross_exp, axis=-1, keepdims=True))).astype(jnp.bfloat16)
    cross_context = jnp.einsum('cht,cthd->chd', cross_weight.astype(jnp.float32), cross_values).reshape(SPANS, D)
    alive = finished == 0
    decoded = jnp.where(alive[:, None], cross_context, 0.0).astype(jnp.bfloat16)
    slot_pos = position[None, :, None]
    length = cache_len[:, None, None]

    def extend(older, fresh):
        grown = jnp.where(slot_pos < length, older, jnp.where(slot_pos == length, fresh[:, None, :], jnp.zeros_like(older)))
        return jnp.where(alive[:, None, None], grown, jnp.zeros_like(older))
    updated = jnp.stack([extend(self_cache[0], token_qkv[1]), extend(self_cache[1], token_qkv[2])])
    moved_cache = jnp.zeros_like(self_cache).at[:, new_slot].set(updated)
    moved_out = jnp.zeros((SPANS, D), jnp.bfloat16).at[new_slot].set(decoded)
    return (moved_cache, moved_out)
```

```python
import collections
import functools

import jax
import jax.numpy as jnp
from jax import lax
from jax.experimental import pallas as pl
from jax.experimental.pallas import tpu as pltpu
from jax.sharding import PartitionSpec as P


HEAD_DIM = 64
RING = 4
SHIFT = 2
TAIL = 8

LIMIT = pltpu.CompilerParams(vmem_limit_bytes=12 * 2**20)
VMEM = pl.BlockSpec(memory_space=pltpu.VMEM)
SMEM = pl.BlockSpec(memory_space=pltpu.SMEM)
HBM = pl.BlockSpec(memory_space=pltpu.HBM)
ANY = pl.BlockSpec(memory_space=pl.ANY)


Plan = collections.namedtuple("Plan", ("local", "stays", "inside", "outside", "place", "turn"))


def moves(new_slot, me, spans, count, j):
    slot = new_slot[j]
    dest = (slot // spans + SHIFT) % count
    mine = (me + SHIFT) % count
    stays = dest == mine
    inside = (dest // RING == mine // RING) & ~stays
    place = dest % RING
    turn = (place - mine % RING + RING) % RING
    return Plan(slot % spans, stays, inside, ~stays & ~inside, place, turn)


def prepare(me_hbm, length_hbm, finished_hbm, slot_hbm, qkv_hbm, cache_hbm, *rest, count):
    updated, chunks, me_ref, length, finished, new_slot, qkv, cache, sems = rest
    pairs = (
        (cache_hbm, cache),
        (me_hbm, me_ref),
        (length_hbm, length),
        (finished_hbm, finished),
        (slot_hbm, new_slot),
        (qkv_hbm, qkv),
    )
    copies = [pltpu.make_async_copy(a, b, sems.at[i]) for i, (a, b) in enumerate(pairs)]
    for copy in copies:
        copy.start()
    for copy in copies:
        copy.wait()
    spans, slots, width = cache.shape[1:]
    me = me_ref[0]
    position = lax.broadcasted_iota(jnp.int32, (slots, width), 0)
    sends = []
    for j in range(spans):
        limit = jnp.where(finished[j] == 0, length[j], -1)
        for a in range(2):
            older = cache[a, j].astype(jnp.float32)
            fresh = qkv[a + 1, j : j + 1].astype(jnp.float32)
            grown = jnp.where(position < limit, older, jnp.where(position == limit, fresh, 0.0))
            updated[j, a * slots : (a + 1) * slots] = grown.astype(jnp.bfloat16)
        plan = moves(new_slot, me, spans, count, j)
        send = pltpu.make_async_copy(updated.at[j], chunks.at[plan.place], sems.at[j])
        sends.append((plan.inside, send))

        @pl.when(plan.inside)
        def _(send=send):
            send.start()

    for inside, send in sends:

        @pl.when(inside)
        def _(send=send):
            send.wait()


def pick(plans, wanted, lines):
    mark = jnp.int32(0)
    line = jnp.zeros_like(lines[0])
    for plan, chosen, candidate in zip(plans, wanted, lines, strict=True):
        mark = jnp.where(chosen, plan.local + 1, mark)
        line = jnp.where(chosen, candidate, line)
    return line, mark.astype(jnp.float32)


def tile_of(line, mark):
    shape = (TAIL, line.shape[1])
    first = lax.broadcasted_iota(jnp.int32, shape, 0) == 0
    return jnp.where(first, jnp.broadcast_to(line, shape), mark).astype(jnp.bfloat16)


def head_rows(row, heads, width):
    head = lax.broadcasted_iota(jnp.int32, (heads, width), 0)
    column = lax.broadcasted_iota(jnp.int32, (heads, width), 1)
    own = column // HEAD_DIM == head
    return own, jnp.where(own, jnp.broadcast_to(row, (heads, width)), 0.0)


def self_attention(length, qkv, cache, proj_hbm, partial, proj, sem):
    copy = pltpu.make_async_copy(proj_hbm, proj, sem)
    copy.start()
    spans, _, width = cache.shape[1:]
    heads = -(-(width // HEAD_DIM) // 8) * 8
    factor = HEAD_DIM ** (-0.5)
    contexts = []
    for j in range(spans):
        query, key, value = (qkv[i, j : j + 1].astype(jnp.float32) for i in range(3))
        own, query_rows = head_rows(query, heads, width)
        scores = (
            lax.dot_general(
                query_rows.astype(jnp.bfloat16), cache[0, j], (((1,), (1,)), ((), ())), preferred_element_type=jnp.float32
            )
            * factor
        )
        usable = lax.broadcasted_iota(jnp.int32, scores.shape, 1) < length[j]
        scores = jnp.where(usable, scores, -1e30)
        own_score = jnp.sum(query_rows * key, axis=1, keepdims=True) * factor
        highest = jnp.maximum(jnp.max(scores, axis=1, keepdims=True), own_score)
        weight = jnp.where(usable, jnp.exp(scores - highest), 0.0)
        own_weight = jnp.exp(own_score - highest)
        total = jnp.sum(weight, axis=1, keepdims=True) + own_weight
        weight = (weight / total).astype(jnp.bfloat16)
        own_weight = (own_weight / total).astype(jnp.bfloat16).astype(jnp.float32)
        mixed = jnp.dot(weight, cache[1, j], preferred_element_type=jnp.float32) + own_weight * value
        contexts.append(jnp.sum(jnp.where(own, mixed, 0.0), axis=0, keepdims=True))
    context = jnp.concatenate(contexts, axis=0).astype(jnp.bfloat16)
    copy.wait()
    partial[...] = jnp.dot(context, proj[...], preferred_element_type=jnp.float32)


def cross_attention(
    me_ref, finished, new_slot, hidden, mine, other, gain, bias, cross, updated, proj_hbm, decoded, near, far1, far2, far3, proj, sem, *, count
):
    copy = pltpu.make_async_copy(proj_hbm, proj, sem)
    copy.start()
    spans, _, width = cross.shape[1:]
    rows = updated.shape[1]
    heads = -(-(width // HEAD_DIM) // 8) * 8
    factor = HEAD_DIM ** (-0.5)
    plans = [moves(new_slot, me_ref[0], spans, count, j) for j in range(spans)]
    parcels = [(block, [p.outside & (p.turn == k) for p in plans]) for k, block in enumerate((far1, far2, far3), 1)]
    for block, wanted in parcels:
        for j, chosen in enumerate(wanted):

            @pl.when(chosen)
            def _(j=j, block=block):
                block[:rows] = updated[j]

    resid = hidden[...].astype(jnp.float32) + (mine[...] + other[...])
    centre = jnp.mean(resid, axis=1, keepdims=True)
    spread = jnp.mean((resid - centre) ** 2, axis=1, keepdims=True)
    normed = ((resid - centre) * lax.rsqrt(spread + 1e-05) * gain[...][None] + bias[...][None]).astype(jnp.bfloat16)
    copy.wait()
    queries = jnp.dot(normed, proj[...], preferred_element_type=jnp.float32).astype(jnp.bfloat16).astype(jnp.float32)
    results = []
    for j in range(spans):
        own, query_rows = head_rows(queries[j : j + 1], heads, width)
        scores = (
            lax.dot_general(
                query_rows.astype(jnp.bfloat16), cross[0, j], (((1,), (1,)), ((), ())), preferred_element_type=jnp.float32
            )
            * factor
        )
        weight = jnp.exp(scores - jnp.max(scores, axis=1, keepdims=True))
        weight = (weight / jnp.sum(weight, axis=1, keepdims=True)).astype(jnp.bfloat16)
        mixed = jnp.dot(weight, cross[1, j], preferred_element_type=jnp.float32)
        result = jnp.sum(jnp.where(own, mixed, 0.0), axis=0, keepdims=True)
        results.append(jnp.where(finished[j] == 0, result, 0.0))
    decoded[...] = jnp.concatenate(results, axis=0).astype(jnp.bfloat16)
    for block, wanted in parcels:
        block[rows:] = tile_of(*pick(plans, wanted, results))
    for x in range(RING):
        near[x] = tile_of(*pick(plans, [p.inside & (p.place == x) for p in plans], results))


def assemble(me_ref, new_slot, updated, decoded, inner, near, got1, got2, got3, moved, moved_out, *, count):
    spans, slots, width = moved.shape[1:]
    rows = 2 * slots
    me = me_ref[0]
    sources = []
    tails = [(near[x], inner.at[x]) for x in range(RING)] + [(got[rows:], got) for got in (got1, got2, got3)]
    for tile, block in tails:
        tile = tile.astype(jnp.float32)
        sources.append((jnp.max(tile[1:, :128]), block, tile[:1]))
    for j in range(spans):
        p = moves(new_slot, me, spans, count, j)
        mark = jnp.where(p.stays, p.local + 1, 0).astype(jnp.float32)
        sources.append((mark, updated.at[j], decoded[j : j + 1].astype(jnp.float32)))
    for l in range(spans):
        row = jnp.zeros((1, width), jnp.float32)
        for mark, block, line in sources:
            chosen = mark == l + 1
            row = jnp.where(chosen, line, row)

            @pl.when(chosen)
            def _(block=block, l=l):
                for a in range(2):
                    moved[a, l] = block[a * slots : (a + 1) * slots]

        moved_out[l : l + 1] = row.astype(jnp.bfloat16)


def here(array):
    return pltpu.with_memory_space_constraint(array, pltpu.VMEM)


def there(array):
    return pltpu.with_memory_space_constraint(array, pltpu.HBM)


def body(hidden, token_qkv, self_cache, cross_kv, cache_len, finished, new_slot, out_proj, ln_gain, ln_bias, query_proj):
    spans, slots, width = self_cache.shape[1:]
    rows = 2 * slots
    count = lax.axis_size("batch")
    cores = lax.axis_size("mp")
    me = lax.axis_index("batch").astype(jnp.int32).reshape(1)
    rings = [[(r * RING + i - SHIFT) % count for i in range(RING)] for r in range(count // RING)]
    bf16 = jnp.bfloat16

    def exchange(chunks):
        return here(lax.all_to_all(chunks, "batch", split_axis=0, concat_axis=0, tiled=True, axis_index_groups=rings))

    def route(k):
        pairs = []
        for i in range(count):
            ring, x = divmod((i + SHIFT) % count, RING)
            to = (x + k) % RING
            pairs.append((i, ((ring + (1 if to < x else -1)) * RING + to - SHIFT) % count))
        return pairs

    block = pltpu.VMEM((rows + TAIL, width), bf16)
    updated, chunks = pl.pallas_call(
        functools.partial(prepare, count=count),
        in_specs=[HBM] * 6,
        out_specs=[VMEM, HBM],
        out_shape=[pltpu.VMEM((spans, rows, width), bf16), pltpu.HBM((RING, rows, width), bf16)],
        scratch_shapes=[pltpu.SMEM((1,), jnp.int32)]
        + [pltpu.SMEM((spans,), jnp.int32)] * 3
        + [pltpu.VMEM(token_qkv.shape, bf16), pltpu.VMEM(self_cache.shape, bf16), pltpu.SemaphoreType.DMA((6,))],
        compiler_params=LIMIT,
        name="prepare",
    )(*map(there, (me, cache_len, finished, new_slot, token_qkv, self_cache)))
    inner = exchange(chunks)
    partial = pl.pallas_call(
        self_attention,
        in_specs=[SMEM, VMEM, VMEM, HBM],
        out_specs=VMEM,
        out_shape=pltpu.VMEM((spans, out_proj.shape[1]), jnp.float32),
        scratch_shapes=[pltpu.VMEM(out_proj.shape, bf16), pltpu.SemaphoreType.DMA],
        compiler_params=LIMIT,
        name="self_attention",
    )(cache_len, token_qkv, self_cache, there(out_proj))
    other = here(lax.ppermute(partial, "mp", [(i, (i + 1) % cores) for i in range(cores)]))
    decoded, near, *far = pl.pallas_call(
        functools.partial(cross_attention, count=count),
        in_specs=[SMEM] * 3 + [VMEM] * 7 + [HBM],
        out_specs=[VMEM] * 5,
        out_shape=[pltpu.VMEM((spans, width), bf16), pltpu.VMEM((RING, TAIL, width), bf16)] + [block] * 3,
        scratch_shapes=[pltpu.VMEM(query_proj.shape, bf16), pltpu.SemaphoreType.DMA],
        compiler_params=LIMIT,
        name="cross_attention",
    )(me, finished, new_slot, hidden, here(partial), other, ln_gain, ln_bias, cross_kv, here(updated), there(query_proj))
    got = []
    for k, sent in enumerate(far, 1):
        got.append(here(lax.ppermute(sent, "batch", route(k))))
    close = exchange(near)
    return pl.pallas_call(
        functools.partial(assemble, count=count),
        in_specs=[SMEM] * 2 + [VMEM] * 7,
        out_specs=[VMEM] * 2,
        out_shape=[jax.ShapeDtypeStruct(self_cache.shape, bf16), jax.ShapeDtypeStruct((spans, width), bf16)],
        compiler_params=LIMIT,
        name="assemble",
    )(me, new_slot, here(updated), here(decoded), inner, close, *got)


def solution(mesh):
    placed = (
        P(("groups", "batch"), None),
        P(None, ("groups", "batch"), "mp"),
        P(None, ("groups", "batch"), None, "mp"),
        P(None, ("groups", "batch"), None, "mp"),
        P(("groups", "batch")),
        P(("groups", "batch")),
        P(("groups", "batch")),
        P("mp", None),
        P(),
        P(),
        P(None, "mp"),
    )

    return jax.shard_map(
        body,
        mesh=mesh,
        in_specs=placed,
        out_specs=(P(None, ("groups", "batch"), None, "mp"), P(("groups", "batch"), "mp")),
        check_vma=False,
    )
```

```python
import collections
import functools

import jax
import jax.numpy as jnp
from jax import lax
from jax.experimental import pallas as pl
from jax.experimental.pallas import tpu as pltpu
from jax.sharding import PartitionSpec as P


HEAD_DIM = 64
RING = 4
SHIFT = 2
TAIL = 8

LIMIT = pltpu.CompilerParams(vmem_limit_bytes=12 * 2**20)
VMEM = pl.BlockSpec(memory_space=pltpu.VMEM)
SMEM = pl.BlockSpec(memory_space=pltpu.SMEM)
HBM = pl.BlockSpec(memory_space=pltpu.HBM)
ANY = pl.BlockSpec(memory_space=pl.ANY)


Plan = collections.namedtuple("Plan", ("local", "stays", "inside", "outside", "place", "turn"))


def moves(new_slot, me, spans, count, j):
    slot = new_slot[j]
    dest = (slot // spans + SHIFT) % count
    mine = (me + SHIFT) % count
    stays = dest == mine
    inside = (dest // RING == mine // RING) & ~stays
    place = dest % RING
    turn = (place - mine % RING + RING) % RING
    return Plan(slot % spans, stays, inside, ~stays & ~inside, place, turn)


def prepare(me_hbm, length_hbm, finished_hbm, slot_hbm, qkv_hbm, cache_hbm, *rest, count):
    updated, kept, chunks, me_ref, length, finished, new_slot, qkv, cache, sems = rest
    spans, slots, width = cache.shape[1:]
    pairs = [(cache_hbm.at[:, j], cache.at[:, j]) for j in range(spans)]
    pairs += [
        (me_hbm, me_ref),
        (length_hbm, length),
        (finished_hbm, finished),
        (slot_hbm, new_slot),
        (qkv_hbm, qkv),
    ]
    copies = [pltpu.make_async_copy(a, b, sems.at[i]) for i, (a, b) in enumerate(pairs)]
    for copy in copies[spans:] + copies[:spans]:
        copy.start()
    for copy in copies[spans:]:
        copy.wait()
    me = me_ref[0]
    position = lax.broadcasted_iota(jnp.int32, (slots, width), 0)
    sends = []
    for j in range(spans):
        copies[j].wait()
        limit = jnp.where(finished[j] == 0, length[j], -1)
        for a in range(2):
            older = cache[a, j].astype(jnp.float32)
            fresh = qkv[a + 1, j : j + 1].astype(jnp.float32)
            grown = jnp.where(position < limit, older, jnp.where(position == limit, fresh, 0.0))
            updated[j, a * slots : (a + 1) * slots] = grown.astype(jnp.bfloat16)
        plan = moves(new_slot, me, spans, count, j)
        mark = jnp.where(plan.stays, plan.local + 1, 0).astype(jnp.float32)
        kept[j] = jnp.full(kept.shape[1:], mark, jnp.float32)
        send = pltpu.make_async_copy(updated.at[j], chunks.at[plan.place], sems.at[j])
        sends.append((plan.inside, send))

        @pl.when(plan.inside)
        def _(send=send):
            send.start()

    for inside, send in sends:

        @pl.when(inside)
        def _(send=send):
            send.wait()


def pick(plans, wanted, lines):
    mark = jnp.int32(0)
    line = jnp.zeros_like(lines[0])
    for plan, chosen, candidate in zip(plans, wanted, lines, strict=True):
        mark = jnp.where(chosen, plan.local + 1, mark)
        line = jnp.where(chosen, candidate, line)
    return line, mark.astype(jnp.float32)


def tile_of(line, mark):
    shape = (TAIL, line.shape[1])
    first = lax.broadcasted_iota(jnp.int32, shape, 0) == 0
    return jnp.where(first, jnp.broadcast_to(line, shape), mark).astype(jnp.bfloat16)


def head_rows(row, heads, width):
    head = lax.broadcasted_iota(jnp.int32, (heads, width), 0)
    column = lax.broadcasted_iota(jnp.int32, (heads, width), 1)
    own = column // HEAD_DIM == head
    return own, jnp.where(own, jnp.broadcast_to(row, (heads, width)), 0.0)


def self_attention(length, qkv, cache, proj_hbm, partial, proj, sem):
    copy = pltpu.make_async_copy(proj_hbm, proj, sem)
    copy.start()
    spans, _, width = cache.shape[1:]
    heads = -(-(width // HEAD_DIM) // 8) * 8
    factor = HEAD_DIM ** (-0.5)
    contexts = []
    for j in range(spans):
        query, key, value = (qkv[i, j : j + 1].astype(jnp.float32) for i in range(3))
        own, query_rows = head_rows(query, heads, width)
        scores = (
            lax.dot_general(
                query_rows.astype(jnp.bfloat16), cache[0, j], (((1,), (1,)), ((), ())), preferred_element_type=jnp.float32
            )
            * factor
        )
        usable = lax.broadcasted_iota(jnp.int32, scores.shape, 1) < length[j]
        scores = jnp.where(usable, scores, -1e30)
        own_score = jnp.sum(query_rows * key, axis=1, keepdims=True) * factor
        highest = jnp.maximum(jnp.max(scores, axis=1, keepdims=True), own_score)
        weight = jnp.where(usable, jnp.exp(scores - highest), 0.0)
        own_weight = jnp.exp(own_score - highest)
        total = jnp.sum(weight, axis=1, keepdims=True) + own_weight
        weight = (weight / total).astype(jnp.bfloat16)
        own_weight = (own_weight / total).astype(jnp.bfloat16).astype(jnp.float32)
        mixed = jnp.dot(weight, cache[1, j], preferred_element_type=jnp.float32) + own_weight * value
        contexts.append(jnp.sum(jnp.where(own, mixed, 0.0), axis=0, keepdims=True))
    context = jnp.concatenate(contexts, axis=0).astype(jnp.bfloat16)
    copy.wait()
    partial[...] = jnp.dot(context, proj[...], preferred_element_type=jnp.float32)


def cross_attention(
    me_ref, finished, new_slot, hidden, mine, other, gain, bias, cross, updated, proj, decoded, near, far1, far2, far3, *, count
):
    spans, _, width = cross.shape[1:]
    rows = updated.shape[1]
    heads = -(-(width // HEAD_DIM) // 8) * 8
    factor = HEAD_DIM ** (-0.5)
    plans = [moves(new_slot, me_ref[0], spans, count, j) for j in range(spans)]
    parcels = [(block, [p.outside & (p.turn == k) for p in plans]) for k, block in enumerate((far1, far2, far3), 1)]
    for block, wanted in parcels:
        for j, chosen in enumerate(wanted):

            @pl.when(chosen)
            def _(j=j, block=block):
                block[:rows] = updated[j]

    resid = hidden[...].astype(jnp.float32) + (mine[...] + other[...])
    centre = jnp.mean(resid, axis=1, keepdims=True)
    spread = jnp.mean((resid - centre) ** 2, axis=1, keepdims=True)
    normed = ((resid - centre) * lax.rsqrt(spread + 1e-05) * gain[...][None] + bias[...][None]).astype(jnp.bfloat16)
    queries = jnp.dot(normed, proj[...], preferred_element_type=jnp.float32).astype(jnp.bfloat16).astype(jnp.float32)
    results = []
    for j in range(spans):
        own, query_rows = head_rows(queries[j : j + 1], heads, width)
        scores = (
            lax.dot_general(
                query_rows.astype(jnp.bfloat16), cross[0, j], (((1,), (1,)), ((), ())), preferred_element_type=jnp.float32
            )
            * factor
        )
        weight = jnp.exp(scores - jnp.max(scores, axis=1, keepdims=True))
        weight = (weight / jnp.sum(weight, axis=1, keepdims=True)).astype(jnp.bfloat16)
        mixed = jnp.dot(weight, cross[1, j], preferred_element_type=jnp.float32)
        result = jnp.sum(jnp.where(own, mixed, 0.0), axis=0, keepdims=True)
        results.append(jnp.where(finished[j] == 0, result, 0.0))
    decoded[...] = jnp.concatenate(results, axis=0).astype(jnp.bfloat16)
    for block, wanted in parcels:
        block[rows:] = tile_of(*pick(plans, wanted, results))
    for x in range(RING):
        near[x] = tile_of(*pick(plans, [p.inside & (p.place == x) for p in plans], results))


def assemble(kept, updated, decoded, inner, near, got1, got2, got3, moved, moved_out):
    spans, slots, width = moved.shape[1:]
    rows = 2 * slots
    tails = [near[x].astype(jnp.float32) for x in range(RING)]
    tails += [got[rows:].astype(jnp.float32) for got in (got1, got2, got3)]
    blocks = [inner.at[x] for x in range(RING)] + [got1, got2, got3] + [updated.at[j] for j in range(spans)]
    found, lines = [], []
    for l in range(spans):
        source = jnp.zeros((1, 128), jnp.float32)
        row = jnp.zeros((1, width), jnp.float32)
        for i, tile in enumerate(tails):
            source = jnp.where(tile[1:2, :128] == l + 1, float(i), source)
            row = jnp.where(tile[1:2] == l + 1, tile[:1], row)
        for j in range(spans):
            source = jnp.where(kept[j, :1, :128] == l + 1, float(len(tails) + j), source)
            row = jnp.where(kept[j, :1] == l + 1, decoded[j : j + 1].astype(jnp.float32), row)
        source = jnp.max(source).astype(jnp.int32)
        found.append(source)
        lines.append(row)
    moved_out[...] = jnp.concatenate(lines, axis=0).astype(jnp.bfloat16)
    for l, source in enumerate(found):
        for i, block in enumerate(blocks):

            @pl.when(source == i)
            def _(block=block, l=l):
                for a in range(2):
                    moved[a, l] = block[a * slots : (a + 1) * slots]


def here(array):
    return pltpu.with_memory_space_constraint(array, pltpu.VMEM)


def there(array):
    return pltpu.with_memory_space_constraint(array, pltpu.HBM)


def body(hidden, token_qkv, self_cache, cross_kv, cache_len, finished, new_slot, out_proj, ln_gain, ln_bias, query_proj):
    spans, slots, width = self_cache.shape[1:]
    rows = 2 * slots
    count = lax.axis_size("batch")
    cores = lax.axis_size("mp")
    me = lax.axis_index("batch").astype(jnp.int32).reshape(1)
    rings = [[(r * RING + i - SHIFT) % count for i in range(RING)] for r in range(count // RING)]
    bf16 = jnp.bfloat16

    def exchange(chunks):
        return here(lax.all_to_all(chunks, "batch", split_axis=0, concat_axis=0, tiled=True, axis_index_groups=rings))

    def route(k):
        pairs = []
        for i in range(count):
            ring, x = divmod((i + SHIFT) % count, RING)
            to = (x + k) % RING
            pairs.append((i, ((ring + (1 if to < x else -1)) * RING + to - SHIFT) % count))
        return pairs

    block = pltpu.VMEM((rows + TAIL, width), bf16)
    updated, kept, chunks = pl.pallas_call(
        functools.partial(prepare, count=count),
        in_specs=[HBM] * 6,
        out_specs=[VMEM, VMEM, HBM],
        out_shape=[
            pltpu.VMEM((spans, rows, width), bf16),
            pltpu.VMEM((spans, TAIL, width), jnp.float32),
            pltpu.HBM((RING, rows, width), bf16),
        ],
        scratch_shapes=[pltpu.SMEM((1,), jnp.int32)]
        + [pltpu.SMEM((spans,), jnp.int32)] * 3
        + [pltpu.VMEM(token_qkv.shape, bf16), pltpu.VMEM(self_cache.shape, bf16), pltpu.SemaphoreType.DMA((5 + spans,))],
        compiler_params=LIMIT,
        name="prepare",
    )(*map(there, (me, cache_len, finished, new_slot, token_qkv, self_cache)))
    inner = exchange(chunks)
    partial = pl.pallas_call(
        self_attention,
        in_specs=[SMEM, VMEM, VMEM, HBM],
        out_specs=VMEM,
        out_shape=pltpu.VMEM((spans, out_proj.shape[1]), jnp.float32),
        scratch_shapes=[pltpu.VMEM(out_proj.shape, bf16), pltpu.SemaphoreType.DMA],
        compiler_params=LIMIT,
        name="self_attention",
    )(cache_len, token_qkv, self_cache, there(out_proj))
    other = here(lax.ppermute(partial, "mp", [(i, (i + 1) % cores) for i in range(cores)]))
    decoded, near, *far = pl.pallas_call(
        functools.partial(cross_attention, count=count),
        in_specs=[SMEM] * 3 + [VMEM] * 8,
        out_specs=[VMEM] * 5,
        out_shape=[pltpu.VMEM((spans, width), bf16), pltpu.VMEM((RING, TAIL, width), bf16)] + [block] * 3,
        compiler_params=LIMIT,
        name="cross_attention",
    )(me, finished, new_slot, hidden, here(partial), other, ln_gain, ln_bias, cross_kv, here(updated), here(query_proj))
    got = []
    for k, sent in enumerate(far, 1):
        got.append(here(lax.ppermute(sent, "batch", route(k))))
    close = exchange(near)
    return pl.pallas_call(
        assemble,
        in_specs=[VMEM] * 8,
        out_specs=[VMEM] * 2,
        out_shape=[jax.ShapeDtypeStruct(self_cache.shape, bf16), jax.ShapeDtypeStruct((spans, width), bf16)],
        compiler_params=LIMIT,
        name="assemble",
    )(here(kept), here(updated), here(decoded), inner, close, *got)


def solution(mesh):
    placed = (
        P(("groups", "batch"), None),
        P(None, ("groups", "batch"), "mp"),
        P(None, ("groups", "batch"), None, "mp"),
        P(None, ("groups", "batch"), None, "mp"),
        P(("groups", "batch")),
        P(("groups", "batch")),
        P(("groups", "batch")),
        P("mp", None),
        P(),
        P(),
        P(None, "mp"),
    )

    return jax.shard_map(
        body,
        mesh=mesh,
        in_specs=placed,
        out_specs=(P(None, ("groups", "batch"), None, "mp"), P(("groups", "batch"), "mp")),
        check_vma=False,
    )
```

```python
import collections
import functools

import jax
import jax.numpy as jnp
from jax import lax
from jax.experimental import pallas as pl
from jax.experimental.pallas import tpu as pltpu
from jax.sharding import PartitionSpec as P


HEAD_DIM = 64
RING = 4
SHIFT = 2
TAIL = 8

LIMIT = pltpu.CompilerParams(vmem_limit_bytes=12 * 2**20)
VMEM = pl.BlockSpec(memory_space=pltpu.VMEM)
SMEM = pl.BlockSpec(memory_space=pltpu.SMEM)
HBM = pl.BlockSpec(memory_space=pltpu.HBM)
ANY = pl.BlockSpec(memory_space=pl.ANY)


Plan = collections.namedtuple("Plan", ("local", "stays", "inside", "outside", "place", "turn"))


def moves(new_slot, me, spans, count, j):
    slot = new_slot[j]
    dest = (slot // spans + SHIFT) % count
    mine = (me + SHIFT) % count
    stays = dest == mine
    inside = (dest // RING == mine // RING) & ~stays
    place = dest % RING
    turn = (place - mine % RING + RING) % RING
    return Plan(slot % spans, stays, inside, ~stays & ~inside, place, turn)


def prepare(me_hbm, length_hbm, finished_hbm, slot_hbm, qkv_hbm, cache_hbm, *rest, count):
    updated, kept, chunks, me_ref, length, finished, new_slot, qkv, cache, sems = rest
    spans, slots, width = cache.shape[1:]
    pairs = [(cache_hbm.at[:, j], cache.at[:, j]) for j in range(spans)]
    pairs += [
        (me_hbm, me_ref),
        (length_hbm, length),
        (finished_hbm, finished),
        (slot_hbm, new_slot),
        (qkv_hbm, qkv),
    ]
    copies = [pltpu.make_async_copy(a, b, sems.at[i]) for i, (a, b) in enumerate(pairs)]
    for copy in copies[spans:] + copies[:spans]:
        copy.start()
    for copy in copies[spans:]:
        copy.wait()
    me = me_ref[0]
    position = lax.broadcasted_iota(jnp.int32, (slots, width), 0)
    sends = []
    for j in range(spans):
        copies[j].wait()
        limit = jnp.where(finished[j] == 0, length[j], -1)
        plan = moves(new_slot, me, spans, count, j)
        mark = jnp.where(plan.stays, plan.local + 1, 0).astype(jnp.float32)
        kept[j] = jnp.full(kept.shape[1:], mark, jnp.float32)
        for a in range(2):
            older = cache[a, j].astype(jnp.float32)
            fresh = qkv[a + 1, j : j + 1].astype(jnp.float32)
            grown = jnp.where(position < limit, older, jnp.where(position == limit, fresh, 0.0))
            half = pl.ds(a * slots, slots)
            updated[j, half] = grown.astype(jnp.bfloat16)
            send = pltpu.make_async_copy(updated.at[j, half], chunks.at[plan.place, half], sems.at[len(copies) + len(sends)])
            sends.append((plan.inside, send))

            @pl.when(plan.inside)
            def _(send=send):
                send.start()

    for inside, send in sends:

        @pl.when(inside)
        def _(send=send):
            send.wait()


def pick(plans, wanted, lines):
    mark = jnp.int32(0)
    line = jnp.zeros_like(lines[0])
    for plan, chosen, candidate in zip(plans, wanted, lines, strict=True):
        mark = jnp.where(chosen, plan.local + 1, mark)
        line = jnp.where(chosen, candidate, line)
    return line, mark.astype(jnp.float32)


def tile_of(line, mark):
    shape = (TAIL, line.shape[1])
    first = lax.broadcasted_iota(jnp.int32, shape, 0) == 0
    return jnp.where(first, jnp.broadcast_to(line, shape), mark).astype(jnp.bfloat16)


def head_rows(row, heads, width):
    head = lax.broadcasted_iota(jnp.int32, (heads, width), 0)
    column = lax.broadcasted_iota(jnp.int32, (heads, width), 1)
    own = column // HEAD_DIM == head
    return own, jnp.where(own, jnp.broadcast_to(row, (heads, width)), 0.0)


def self_attention(length, qkv, cache, proj_hbm, partial, proj, sem):
    copy = pltpu.make_async_copy(proj_hbm, proj, sem)
    copy.start()
    spans, _, width = cache.shape[1:]
    heads = -(-(width // HEAD_DIM) // 8) * 8
    factor = HEAD_DIM ** (-0.5)
    contexts = []
    for j in range(spans):
        query, key, value = (qkv[i, j : j + 1].astype(jnp.float32) for i in range(3))
        own, query_rows = head_rows(query, heads, width)
        scores = (
            lax.dot_general(
                query_rows.astype(jnp.bfloat16), cache[0, j], (((1,), (1,)), ((), ())), preferred_element_type=jnp.float32
            )
            * factor
        )
        usable = lax.broadcasted_iota(jnp.int32, scores.shape, 1) < length[j]
        scores = jnp.where(usable, scores, -1e30)
        own_score = jnp.sum(query_rows * key, axis=1, keepdims=True) * factor
        highest = jnp.maximum(jnp.max(scores, axis=1, keepdims=True), own_score)
        weight = jnp.where(usable, jnp.exp(scores - highest), 0.0)
        own_weight = jnp.exp(own_score - highest)
        total = jnp.sum(weight, axis=1, keepdims=True) + own_weight
        weight = (weight / total).astype(jnp.bfloat16)
        own_weight = (own_weight / total).astype(jnp.bfloat16).astype(jnp.float32)
        mixed = jnp.dot(weight, cache[1, j], preferred_element_type=jnp.float32) + own_weight * value
        contexts.append(jnp.sum(jnp.where(own, mixed, 0.0), axis=0, keepdims=True))
    context = jnp.concatenate(contexts, axis=0).astype(jnp.bfloat16)
    copy.wait()
    partial[...] = jnp.dot(context, proj[...], preferred_element_type=jnp.float32)


def cross_attention(
    me_ref, finished, new_slot, hidden, mine, other, gain, bias, cross, updated, proj, decoded, near, far1, far2, far3, *, count
):
    spans, _, width = cross.shape[1:]
    rows = updated.shape[1]
    heads = -(-(width // HEAD_DIM) // 8) * 8
    factor = HEAD_DIM ** (-0.5)
    plans = [moves(new_slot, me_ref[0], spans, count, j) for j in range(spans)]
    parcels = [(block, [p.outside & (p.turn == k) for p in plans]) for k, block in enumerate((far1, far2, far3), 1)]
    for block, wanted in parcels:
        for j, chosen in enumerate(wanted):

            @pl.when(chosen)
            def _(j=j, block=block):
                block[:rows] = updated[j]

    resid = hidden[...].astype(jnp.float32) + (mine[...] + other[...])
    centre = jnp.mean(resid, axis=1, keepdims=True)
    spread = jnp.mean((resid - centre) ** 2, axis=1, keepdims=True)
    normed = ((resid - centre) * lax.rsqrt(spread + 1e-05) * gain[...][None] + bias[...][None]).astype(jnp.bfloat16)
    queries = jnp.dot(normed, proj[...], preferred_element_type=jnp.float32).astype(jnp.bfloat16).astype(jnp.float32)
    results = []
    for j in range(spans):
        own, query_rows = head_rows(queries[j : j + 1], heads, width)
        scores = (
            lax.dot_general(
                query_rows.astype(jnp.bfloat16), cross[0, j], (((1,), (1,)), ((), ())), preferred_element_type=jnp.float32
            )
            * factor
        )
        weight = jnp.exp(scores - jnp.max(scores, axis=1, keepdims=True))
        weight = (weight / jnp.sum(weight, axis=1, keepdims=True)).astype(jnp.bfloat16)
        mixed = jnp.dot(weight, cross[1, j], preferred_element_type=jnp.float32)
        result = jnp.sum(jnp.where(own, mixed, 0.0), axis=0, keepdims=True)
        results.append(jnp.where(finished[j] == 0, result, 0.0))
    decoded[...] = jnp.concatenate(results, axis=0).astype(jnp.bfloat16)
    for block, wanted in parcels:
        block[rows:] = tile_of(*pick(plans, wanted, results))
    for x in range(RING):
        near[x] = tile_of(*pick(plans, [p.inside & (p.place == x) for p in plans], results))


def assemble(kept, updated, decoded, inner, near, got1, got2, got3, moved, moved_out):
    spans, slots, width = moved.shape[1:]
    rows = 2 * slots
    tails = [near[x].astype(jnp.float32) for x in range(RING)]
    tails += [got[rows:].astype(jnp.float32) for got in (got1, got2, got3)]
    blocks = [inner.at[x] for x in range(RING)] + [got1, got2, got3] + [updated.at[j] for j in range(spans)]
    found, lines = [], []
    for l in range(spans):
        source = jnp.zeros((1, 128), jnp.float32)
        row = jnp.zeros((1, width), jnp.float32)
        for i, tile in enumerate(tails):
            source = jnp.where(tile[1:2, :128] == l + 1, float(i), source)
            row = jnp.where(tile[1:2] == l + 1, tile[:1], row)
        for j in range(spans):
            source = jnp.where(kept[j, :1, :128] == l + 1, float(len(tails) + j), source)
            row = jnp.where(kept[j, :1] == l + 1, decoded[j : j + 1].astype(jnp.float32), row)
        source = jnp.max(source).astype(jnp.int32)
        found.append(source)
        lines.append(row)
    moved_out[...] = jnp.concatenate(lines, axis=0).astype(jnp.bfloat16)
    for l, source in enumerate(found):
        for i, block in enumerate(blocks):

            @pl.when(source == i)
            def _(block=block, l=l):
                for a in range(2):
                    moved[a, l] = block[a * slots : (a + 1) * slots]


def here(array):
    return pltpu.with_memory_space_constraint(array, pltpu.VMEM)


def there(array):
    return pltpu.with_memory_space_constraint(array, pltpu.HBM)


def body(hidden, token_qkv, self_cache, cross_kv, cache_len, finished, new_slot, out_proj, ln_gain, ln_bias, query_proj):
    spans, slots, width = self_cache.shape[1:]
    rows = 2 * slots
    count = lax.axis_size("batch")
    cores = lax.axis_size("mp")
    me = lax.axis_index("batch").astype(jnp.int32).reshape(1)
    rings = [[(r * RING + i - SHIFT) % count for i in range(RING)] for r in range(count // RING)]
    bf16 = jnp.bfloat16

    def exchange(chunks):
        return here(lax.all_to_all(chunks, "batch", split_axis=0, concat_axis=0, tiled=True, axis_index_groups=rings))

    def route(k):
        pairs = []
        for i in range(count):
            ring, x = divmod((i + SHIFT) % count, RING)
            to = (x + k) % RING
            pairs.append((i, ((ring + (1 if to < x else -1)) * RING + to - SHIFT) % count))
        return pairs

    block = pltpu.VMEM((rows + TAIL, width), bf16)
    updated, kept, chunks = pl.pallas_call(
        functools.partial(prepare, count=count),
        in_specs=[HBM] * 6,
        out_specs=[VMEM, VMEM, HBM],
        out_shape=[
            pltpu.VMEM((spans, rows, width), bf16),
            pltpu.VMEM((spans, TAIL, width), jnp.float32),
            pltpu.HBM((RING, rows, width), bf16),
        ],
        scratch_shapes=[pltpu.SMEM((1,), jnp.int32)]
        + [pltpu.SMEM((spans,), jnp.int32)] * 3
        + [pltpu.VMEM(token_qkv.shape, bf16), pltpu.VMEM(self_cache.shape, bf16), pltpu.SemaphoreType.DMA((5 + 3 * spans,))],
        compiler_params=LIMIT,
        name="prepare",
    )(*map(there, (me, cache_len, finished, new_slot, token_qkv, self_cache)))
    inner = exchange(chunks)
    partial = pl.pallas_call(
        self_attention,
        in_specs=[SMEM, VMEM, VMEM, HBM],
        out_specs=VMEM,
        out_shape=pltpu.VMEM((spans, out_proj.shape[1]), jnp.float32),
        scratch_shapes=[pltpu.VMEM(out_proj.shape, bf16), pltpu.SemaphoreType.DMA],
        compiler_params=LIMIT,
        name="self_attention",
    )(cache_len, token_qkv, self_cache, there(out_proj))
    other = here(lax.ppermute(partial, "mp", [(i, (i + 1) % cores) for i in range(cores)]))
    decoded, near, *far = pl.pallas_call(
        functools.partial(cross_attention, count=count),
        in_specs=[SMEM] * 3 + [VMEM] * 8,
        out_specs=[VMEM] * 5,
        out_shape=[pltpu.VMEM((spans, width), bf16), pltpu.VMEM((RING, TAIL, width), bf16)] + [block] * 3,
        compiler_params=LIMIT,
        name="cross_attention",
    )(me, finished, new_slot, hidden, here(partial), other, ln_gain, ln_bias, cross_kv, here(updated), here(query_proj))
    got = []
    for k, sent in enumerate(far, 1):
        got.append(here(lax.ppermute(sent, "batch", route(k))))
    close = exchange(near)
    return pl.pallas_call(
        assemble,
        in_specs=[VMEM] * 8,
        out_specs=[VMEM] * 2,
        out_shape=[jax.ShapeDtypeStruct(self_cache.shape, bf16), jax.ShapeDtypeStruct((spans, width), bf16)],
        compiler_params=LIMIT,
        name="assemble",
    )(here(kept), here(updated), here(decoded), inner, close, *got)


def solution(mesh):
    placed = (
        P(("groups", "batch"), None),
        P(None, ("groups", "batch"), "mp"),
        P(None, ("groups", "batch"), None, "mp"),
        P(None, ("groups", "batch"), None, "mp"),
        P(("groups", "batch")),
        P(("groups", "batch")),
        P(("groups", "batch")),
        P("mp", None),
        P(),
        P(),
        P(None, "mp"),
    )

    return jax.shard_map(
        body,
        mesh=mesh,
        in_specs=placed,
        out_specs=(P(None, ("groups", "batch"), None, "mp"), P(("groups", "batch"), "mp")),
        check_vma=False,
    )
```
